32 devices in a mesh: rep: 8 (over y, x, core), tp: 4 (over z).
Axes of the slice: x: 2, y: 2, z: 4, core: 2. Of those that a mesh axis runs over, the one named last changes fastest.
Arguments:
- queries: bfloat16 [2048, 4096], P('rep', 'tp'), may hold values from -120 to 120
- keys_new: bfloat16 [2048, 1024], P('rep', 'tp'), may hold values from -7 to 7
- values_new: bfloat16 [2048, 1024], P('rep', 'tp'), may hold values from -6 to 6
- caches: bfloat16 [16, 2, 4096, 1024], P('rep', None, None, 'tp'), may hold values from -6 to 6
- lengths: int32 [8, 2], replicated, may hold values from 128 to 4096, as said below
- moving: int32 [8], replicated, may hold values from 0 to 1
- destination: int32 [8], replicated, may hold values from 0 to 7, each once
- out_weight: bfloat16 [4096, 4096], P('tp'), may hold values from -0.09375 to 0.09375
Outputs:
- mixed: bfloat16 [2048, 4096], P('rep', 'tp')
- held_cache: bfloat16 [16, 2, 4096, 1024], P('rep', None, None, 'tp')
The draws below stay inside these ranges and needn't reach their ends.
Inputs may be any that keep to these rules, and one draw needn't show every extreme that they name: `lengths`: multiples of 128; in every draw some slot holds 4096 and some 128. `destination`: each replica receives exactly one failing candidate; it takes the slot that its own failing candidate leaves.
All inputs are finite; a program needn't handle non-finite values.
Results may differ from the reference program's by a relative error of at most 0.014.
Values may be sent and summed in bfloat16 or wider, within the bound.
A program may use at most 64 MiB of HBM per device.

```python
import jax
import jax.numpy as jnp
from jax import lax

HEADS = 32
KV_HEADS = 8
HEAD = 128
OUT = 4096
SPAN = 128
SLOTS = 2
CACHE = 4096
ROWS = 2048
N_REP = 8


def fresh_keys(key):
    base = jax.random.normal(jax.random.fold_in(key, 7), (ROWS, KV_HEADS, HEAD), jnp.float32)
    return jnp.clip(base, -6.0, 6.0)


def draw_keys_new(key, part):
    base = fresh_keys(key)
    return base.reshape(ROWS, KV_HEADS * HEAD).astype(jnp.bfloat16)


def draw_queries(key, part):
    base = jnp.clip(jax.random.normal(jax.random.fold_in(key, 11), (ROWS, HEADS, HEAD), jnp.float32), -6.0, 6.0)
    return base.reshape(ROWS, HEADS * HEAD).astype(jnp.bfloat16)


def draw_lengths(key, part):
    blocks = jax.random.randint(jax.random.fold_in(key, 3), (N_REP * SLOTS,), 1, CACHE // 128 + 1)
    picked = jax.random.permutation(jax.random.fold_in(key, 5), N_REP * SLOTS)
    blocks = blocks.at[picked[0]].set(CACHE // 128)
    blocks = blocks.at[picked[1]].set(1)
    return (blocks * 128).reshape(N_REP, SLOTS).astype(jnp.int32)


def with_ends(values, stream_key, smallest, high):
    spot = [jax.random.randint(jax.random.fold_in(stream_key, axis), (), 0, length) for axis, length in enumerate(values.shape)]
    longest = values.shape.index(max(values.shape))
    beside = spot[:longest] + [(spot[longest] + 1) % values.shape[longest]] + spot[longest + 1:]
    return values.at[tuple(spot)].set(smallest).at[tuple(beside)].set(high)


def level_of(own_key, extent, pieces, least, top_value):
    def one(dim, shards_of):
        heights = jax.random.uniform(jax.random.fold_in(jax.random.fold_in(own_key, 6), dim), (shards_of,), jnp.float32, least / len(pieces), top_value / len(pieces))
        return jnp.repeat(jnp.exp(heights), extent[dim] // shards_of).reshape((-1,) + (1,) * (len(extent) - dim - 1))

    gain = one(*pieces[0])
    for cut in pieces[1:]:
        gain = gain * one(*cut)
    return gain


def gaussian(rng, dims, deviation, reach, pieces=(), kind=jnp.bfloat16):
    level = level_of(rng, dims, pieces, -0.22, 0.18) if pieces else 1.0
    drawn = jax.random.normal(rng, dims, jnp.float32) * deviation * level
    return jnp.minimum(jnp.maximum(drawn, -reach), reach).astype(kind)


def setup_inputs(seed: int = 0) -> dict:
    streams_of = jax.random.split(jax.random.key(seed), 9)
    queries = draw_queries(jax.random.fold_in(streams_of[8], 71), 0)
    keys_new = draw_keys_new(jax.random.fold_in(streams_of[8], 71), 0)
    values_new = gaussian(streams_of[2], (ROWS, KV_HEADS * HEAD), 1.0, 6.0, ((0, 8), (1, 4)))
    caches = gaussian(streams_of[3], (N_REP * SLOTS, 2, CACHE, KV_HEADS * HEAD), 1.0, 6.0, ((0, 8), (3, 4)))
    lengths = draw_lengths(jax.random.fold_in(streams_of[8], 71), 0)
    moving = with_ends(jax.random.randint(streams_of[5], (N_REP,), 0, SLOTS), jax.random.fold_in(streams_of[5], 1), 0, SLOTS - 1).astype(jnp.int32)
    destination = jax.random.permutation(streams_of[6], N_REP).astype(jnp.int32)
    out_weight = gaussian(streams_of[7], (HEADS * HEAD, OUT), (HEADS * HEAD) ** -0.5, 0.09375, ((0, 4),))
    return {"queries": queries, "keys_new": keys_new, "values_new": values_new, "caches": caches, "lengths": lengths, "moving": moving, "destination": destination, "out_weight": out_weight}


masked_score = -1e30
key_block_rows = 512


def product(form, left, right):
    return jnp.einsum(form, left.astype(jnp.float32), right.astype(jnp.float32))


def attend(query_slot, key_cache, value_cache, length, keys_fresh, values_fresh, block_count):
    span_rows = query_slot.shape[0]
    kv_count = key_cache.shape[1] // HEAD
    group_size = query_slot.shape[1] // (HEAD * kv_count)
    grouped = query_slot.reshape(span_rows, kv_count, group_size, HEAD).transpose(1, 2, 0, 3)
    grouped = grouped.reshape(kv_count, group_size * span_rows, HEAD)
    scale = HEAD ** -0.5
    token_of_row = jnp.arange(group_size * span_rows, dtype=jnp.int32) % span_rows

    def absorb(running, key_block, value_block, visible):
        row_max, row_total, weighted = running
        scores = product('gqd,kgd->gqk', grouped, key_block) * scale
        scores = jnp.where(visible, scores, masked_score)
        new_max = jnp.maximum(row_max, jnp.max(scores, axis=2))
        rescale = jnp.exp(row_max - new_max)
        weights_block = jnp.where(visible, jnp.exp(scores - new_max[:, :, None]), 0.0)
        row_total = row_total * rescale + jnp.sum(weights_block, axis=2)
        rounded = lax.optimization_barrier(weights_block.astype(jnp.bfloat16))
        weighted = weighted * rescale[:, :, None] + product('gqk,kgd->gqd', rounded, value_block)
        return new_max, row_total, weighted

    def cache_step(block_index, running):
        start = block_index * key_block_rows
        key_block = lax.dynamic_slice_in_dim(key_cache, start, key_block_rows, 0).reshape(key_block_rows, kv_count, HEAD)
        value_block = lax.dynamic_slice_in_dim(value_cache, start, key_block_rows, 0).reshape(key_block_rows, kv_count, HEAD)
        visible = (start + jnp.arange(key_block_rows, dtype=jnp.int32) < length)[None, None, :]
        return absorb(running, key_block, value_block, visible)

    rows_all = group_size * span_rows
    initial = (jnp.full((kv_count, rows_all), masked_score, jnp.float32),
               jnp.zeros((kv_count, rows_all), jnp.float32),
               jnp.zeros((kv_count, rows_all, HEAD), jnp.float32))
    running = lax.fori_loop(0, block_count, cache_step, initial)
    visible = (jnp.arange(span_rows, dtype=jnp.int32)[None, :] <= token_of_row[:, None])[None]
    running = absorb(running, keys_fresh.reshape(span_rows, kv_count, HEAD),
                     values_fresh.reshape(span_rows, kv_count, HEAD), visible)
    result = running[2] / running[1][:, :, None]
    result = result.reshape(kv_count, group_size, span_rows, HEAD).transpose(2, 0, 1, 3)
    return result.reshape(span_rows, kv_count * group_size * HEAD).astype(jnp.bfloat16)


def reference(queries, keys_new, values_new, caches, lengths, moving, destination, out_weight):
    source_of = jnp.argsort(destination).astype(jnp.int32)
    flat_lengths = lengths.reshape(-1)
    slot_indices = jnp.arange(N_REP * SLOTS, dtype=jnp.int32)
    replica_of = slot_indices // SLOTS
    number_of = slot_indices % SLOTS
    anchor_of = source_of[replica_of]
    taken_all = jnp.where(number_of == moving[replica_of], anchor_of * SLOTS + moving[anchor_of],
                          slot_indices).astype(jnp.int32)
    held_cache = jnp.take(caches, taken_all, axis=0)

    def per_slot(slot_index):
        taken = taken_all[slot_index]
        cache_slot = lax.dynamic_index_in_dim(held_cache, slot_index, 0, keepdims=False)
        length = flat_lengths[taken]
        start = (slot_index * SPAN).astype(jnp.int32)
        query_slot = lax.dynamic_slice_in_dim(queries, start, SPAN, 0)
        keys_fresh = lax.dynamic_slice_in_dim(keys_new, start, SPAN, 0)
        values_fresh = lax.dynamic_slice_in_dim(values_new, start, SPAN, 0)
        return attend(query_slot, cache_slot[0], cache_slot[1], length, keys_fresh, values_fresh, CACHE // key_block_rows)

    attended = lax.map(per_slot, slot_indices)
    attended = attended.reshape(N_REP * SLOTS * SPAN, HEADS * HEAD)
    mixed = jnp.dot(attended, out_weight, preferred_element_type=jnp.float32).astype(jnp.bfloat16)
    return (mixed, held_cache)
```

```python
import functools

import jax
import jax.numpy as jnp
from jax import lax
from jax.experimental import pallas as pl
from jax.experimental.pallas import tpu as pltpu
from jax.sharding import PartitionSpec as P

HEAD = 128
BLOCK = 512
LOG2E = 1.4426950408889634
masked_score = -1e30


def slot_kernel(
    scalars, source, query_t, keys_fresh, values_fresh, *rest, aliased, kv_count, group
):
    if aliased:
        rest = rest[1:]
    held, attended, cache, row_max, row_total, weighted, in_sem, out_sem = rest
    taken, target, length = scalars[0], scalars[1], scalars[2]
    rows = cache.shape[1]
    blocks = rows // BLOCK
    span = keys_fresh.shape[0]
    factor = HEAD ** (-0.5) * LOG2E

    def fetch(block, part):
        at = pl.ds(pl.multiple_of(block * BLOCK, BLOCK), BLOCK)
        return pltpu.make_async_copy(
            source.at[taken, part, at], cache.at[part, at], in_sem.at[block, part]
        )

    def put(block, part):
        at = pl.ds(pl.multiple_of(block * BLOCK, BLOCK), BLOCK)
        return pltpu.make_async_copy(
            cache.at[part, at], held.at[target, part, at], out_sem.at[block, part]
        )

    for block in range(blocks):
        for part in range(2):
            fetch(block, part).start()

    def scores_of(head, keys):
        return lax.dot_general(
            keys,
            query_t[head],
            (((1,), (0,)), ((), ())),
            preferred_element_type=jnp.float32,
        )

    def mix(values, weights):
        return lax.dot_general(
            values,
            weights.astype(jnp.bfloat16),
            (((0,), (0,)), ((), ())),
            preferred_element_type=jnp.float32,
        )

    key_at = lax.broadcasted_iota(jnp.int32, (span, group * span), 0)
    token_at = lax.broadcasted_iota(jnp.int32, (span, group * span), 1) % span
    for head in range(kv_count):
        lanes = slice(head * HEAD, (head + 1) * HEAD)
        scores = jnp.where(
            key_at <= token_at, scores_of(head, keys_fresh[:, lanes]), masked_score
        )
        new_max = jnp.max(scores, axis=0, keepdims=True)
        weights = jnp.exp2((scores - new_max) * factor)
        row_max[head] = new_max
        row_total[head] = jnp.sum(weights, axis=0, keepdims=True)
        weighted[head] = mix(values_fresh[:, lanes], weights)

    def absorb(block, masked):
        start = pl.multiple_of(block * BLOCK, BLOCK)
        at = pl.ds(start, BLOCK)
        for head in range(kv_count):
            lanes = slice(head * HEAD, (head + 1) * HEAD)
            scores = scores_of(head, cache[0, at, lanes])
            if masked:
                position = start + lax.broadcasted_iota(jnp.int32, scores.shape, 0)
                scores = jnp.where(position < length, scores, masked_score)
            old_max = row_max[head]
            new_max = jnp.maximum(old_max, jnp.max(scores, axis=0, keepdims=True))
            rescale = jnp.exp2((old_max - new_max) * factor)
            weights = jnp.exp2((scores - new_max) * factor)
            row_max[head] = new_max
            row_total[head] = row_total[head] * rescale + jnp.sum(
                weights, axis=0, keepdims=True
            )
            weighted[head] = weighted[head] * rescale + mix(cache[1, at, lanes], weights)

    def step(block, carry):
        for part in range(2):
            fetch(block, part).wait()
            put(block, part).start()
        start = block * BLOCK

        @pl.when(start + BLOCK <= length)
        def _():
            absorb(block, False)

        @pl.when((start < length) & (length < start + BLOCK))
        def _():
            absorb(block, True)

        return carry

    lax.fori_loop(0, blocks, step, 0)
    for head in range(kv_count):
        result = (weighted[head] / row_total[head]).T
        for member in range(group):
            lanes = slice((head * group + member) * HEAD, (head * group + member + 1) * HEAD)
            attended[:, lanes] = result[member * span : (member + 1) * span].astype(
                jnp.bfloat16
            )
    for block in range(blocks):
        for part in range(2):
            put(block, part).wait()


def attend_slot(scalars, source, query_t, keys_fresh, values_fresh, held, held_shape):
    kv_count, _, columns = query_t.shape
    span = keys_fresh.shape[0]
    group = columns // span
    rows, width = source.shape[2:]
    aliased = held is not None
    anywhere = pl.BlockSpec(memory_space=pl.ANY)
    vmem = pl.BlockSpec(memory_space=pltpu.VMEM)
    operands = [scalars, source, query_t, keys_fresh, values_fresh]
    in_specs = [pl.BlockSpec(memory_space=pltpu.SMEM), anywhere, vmem, vmem, vmem]
    if aliased:
        operands.append(held)
        in_specs.append(anywhere)
    blocks = rows // BLOCK
    return pl.pallas_call(
        functools.partial(slot_kernel, aliased=aliased, kv_count=kv_count, group=group),
        out_shape=(
            jax.ShapeDtypeStruct(held_shape, jnp.bfloat16),
            jax.ShapeDtypeStruct((span, kv_count * group * HEAD), jnp.bfloat16),
        ),
        in_specs=in_specs,
        out_specs=(anywhere, vmem),
        scratch_shapes=[
            pltpu.VMEM((2, rows, width), jnp.bfloat16),
            pltpu.VMEM((kv_count, 1, columns), jnp.float32),
            pltpu.VMEM((kv_count, 1, columns), jnp.float32),
            pltpu.VMEM((kv_count, HEAD, columns), jnp.float32),
            pltpu.SemaphoreType.DMA((blocks, 2)),
            pltpu.SemaphoreType.DMA((blocks, 2)),
        ],
        input_output_aliases={5: 0} if aliased else {},
        compiler_params=pltpu.CompilerParams(vmem_limit_bytes=40 * 1024 * 1024),
        cost_estimate=pl.CostEstimate(
            flops=4 * kv_count * columns * (rows + span) * HEAD,
            bytes_accessed=8 * rows * width,
            transcendentals=kv_count * columns * (rows + span),
        ),
    )(*operands)


def on_device(queries, keys_new, values_new, caches, lengths, moving, destination, out_weight):
    replicas = lax.axis_size("rep")
    own_index = lax.axis_index("rep")
    slot_count, _, cache_rows, width = caches.shape
    span = queries.shape[0] // slot_count
    kv_count = width // HEAD
    group = queries.shape[1] // width
    leaving_slot = moving[own_index]
    staying_slot = 1 - leaving_slot
    leaving = lax.dynamic_index_in_dim(caches, leaving_slot, 0, keepdims=False)
    piece_rows = 2 * cache_rows // replicas
    pieces = leaving.reshape(replicas, piece_rows, width)
    spread = lax.all_to_all(pieces, "rep", split_axis=0, concat_axis=0, tiled=True)
    source_of = jnp.argsort(destination)
    ordered = jnp.take(spread, source_of, axis=0, mode="clip")
    arrived = lax.all_to_all(ordered, "rep", split_axis=0, concat_axis=0, tiled=True)
    arrived = arrived.reshape(1, 2, cache_rows, width)

    anchor = source_of[own_index]
    incoming_length = lengths[anchor, moving[anchor]]
    staying_length = lengths[own_index, staying_slot]
    query_t = (
        queries.reshape(slot_count, span, kv_count, group, HEAD)
        .transpose(0, 2, 4, 3, 1)
        .reshape(slot_count, kv_count, HEAD, group * span)
    )
    keys_by_slot = keys_new.reshape(slot_count, span, width)
    values_by_slot = values_new.reshape(slot_count, span, width)

    def pick(array, slot):
        return lax.dynamic_index_in_dim(array, slot, 0, keepdims=False)

    def project(attended):
        partial_value = jnp.dot(attended, out_weight, preferred_element_type=jnp.float32)
        return lax.psum_scatter(
            partial_value.astype(jnp.bfloat16), "tp", scatter_dimension=1, tiled=True
        )

    held, staying_attended = attend_slot(
        jnp.stack([staying_slot, staying_slot, staying_length]),
        caches,
        pick(query_t, staying_slot),
        pick(keys_by_slot, staying_slot),
        pick(values_by_slot, staying_slot),
        None,
        caches.shape,
    )
    staying_mixed = project(staying_attended)
    held, arrived_attended = attend_slot(
        jnp.stack([jnp.zeros_like(leaving_slot), leaving_slot, incoming_length]),
        arrived,
        pick(query_t, leaving_slot),
        pick(keys_by_slot, leaving_slot),
        pick(values_by_slot, leaving_slot),
        held,
        caches.shape,
    )
    arrived_mixed = project(arrived_attended)
    mixed = jnp.where(
        leaving_slot == 0,
        jnp.concatenate([arrived_mixed, staying_mixed], axis=0),
        jnp.concatenate([staying_mixed, arrived_mixed], axis=0),
    )
    return (mixed, held)


def solution(mesh):
    in_specs = (
        P("rep", "tp"),
        P("rep", "tp"),
        P("rep", "tp"),
        P("rep", None, None, "tp"),
        P(),
        P(),
        P(),
        P("tp", None),
    )
    out_specs = (P("rep", "tp"), P("rep", None, None, "tp"))
    return jax.shard_map(
        on_device, mesh=mesh, in_specs=in_specs, out_specs=out_specs, check_vma=False
    )
```

```python
import functools

import jax
import jax.numpy as jnp
from jax import lax
from jax.experimental import pallas as pl
from jax.experimental.pallas import tpu as pltpu
from jax.sharding import PartitionSpec as P

HEAD = 128
BLOCK = 512
LOG2E = 1.4426950408889634
masked_score = -1e30


def slot_kernel(
    scalars, source, query_t, keys_fresh, values_fresh, *rest, aliased, kv_count, group
):
    if aliased:
        rest = rest[1:]
    held, attended, cache, row_max, row_total, weighted, in_sem, out_sem = rest
    taken, target, length = scalars[0], scalars[1], scalars[2]
    rows = cache.shape[1]
    blocks = rows // BLOCK
    span = keys_fresh.shape[0]
    factor = HEAD ** (-0.5) * LOG2E

    def fetch(block, part):
        at = pl.ds(pl.multiple_of(block * BLOCK, BLOCK), BLOCK)
        return pltpu.make_async_copy(
            source.at[taken, part, at], cache.at[part, at], in_sem.at[block, part]
        )

    def put(block, part):
        at = pl.ds(pl.multiple_of(block * BLOCK, BLOCK), BLOCK)
        return pltpu.make_async_copy(
            cache.at[part, at], held.at[target, part, at], out_sem.at[block, part]
        )

    for block in range(blocks):
        for part in range(2):
            fetch(block, part).start()

    def scores_of(head, keys):
        return lax.dot_general(
            keys,
            query_t[head],
            (((1,), (0,)), ((), ())),
            preferred_element_type=jnp.float32,
        )

    def mix(values, weights):
        return lax.dot_general(
            values,
            weights.astype(jnp.bfloat16),
            (((0,), (0,)), ((), ())),
            preferred_element_type=jnp.float32,
        )

    key_at = lax.broadcasted_iota(jnp.int32, (span, group * span), 0)
    token_at = lax.broadcasted_iota(jnp.int32, (span, group * span), 1) % span
    for head in range(kv_count):
        lanes = slice(head * HEAD, (head + 1) * HEAD)
        scores = jnp.where(
            key_at <= token_at, scores_of(head, keys_fresh[:, lanes]), masked_score
        )
        new_max = jnp.max(scores, axis=0, keepdims=True)
        weights = jnp.exp2((scores - new_max) * factor)
        row_max[head] = new_max
        row_total[head] = jnp.sum(weights, axis=0, keepdims=True)
        weighted[head] = mix(values_fresh[:, lanes], weights)

    def absorb(block, masked):
        start = pl.multiple_of(block * BLOCK, BLOCK)
        at = pl.ds(start, BLOCK)
        for head in range(kv_count):
            lanes = slice(head * HEAD, (head + 1) * HEAD)
            scores = scores_of(head, cache[0, at, lanes])
            if masked:
                position = start + lax.broadcasted_iota(jnp.int32, scores.shape, 0)
                scores = jnp.where(position < length, scores, masked_score)
            old_max = row_max[head]
            new_max = jnp.maximum(old_max, jnp.max(scores, axis=0, keepdims=True))
            rescale = jnp.exp2((old_max - new_max) * factor)
            weights = jnp.exp2((scores - new_max) * factor)
            row_max[head] = new_max
            row_total[head] = row_total[head] * rescale + jnp.sum(
                weights, axis=0, keepdims=True
            )
            weighted[head] = weighted[head] * rescale + mix(cache[1, at, lanes], weights)

    def step(block, carry):
        for part in range(2):
            fetch(block, part).wait()
            put(block, part).start()
        start = block * BLOCK

        @pl.when(start + BLOCK <= length)
        def _():
            absorb(block, False)

        @pl.when((start < length) & (length < start + BLOCK))
        def _():
            absorb(block, True)

        return carry

    lax.fori_loop(0, blocks, step, 0)
    for head in range(kv_count):
        result = (weighted[head] / row_total[head]).T
        for member in range(group):
            lanes = slice((head * group + member) * HEAD, (head * group + member + 1) * HEAD)
            attended[:, lanes] = result[member * span : (member + 1) * span].astype(
                jnp.bfloat16
            )
    for block in range(blocks):
        for part in range(2):
            put(block, part).wait()


def attend_slot(scalars, source, query_t, keys_fresh, values_fresh, held, held_shape):
    kv_count, _, columns = query_t.shape
    span = keys_fresh.shape[0]
    group = columns // span
    rows, width = source.shape[2:]
    aliased = held is not None
    anywhere = pl.BlockSpec(memory_space=pl.ANY)
    vmem = pl.BlockSpec(memory_space=pltpu.VMEM)
    operands = [scalars, source, query_t, keys_fresh, values_fresh]
    in_specs = [pl.BlockSpec(memory_space=pltpu.SMEM), anywhere, vmem, vmem, vmem]
    if aliased:
        operands.append(held)
        in_specs.append(anywhere)
    blocks = rows // BLOCK
    return pl.pallas_call(
        functools.partial(slot_kernel, aliased=aliased, kv_count=kv_count, group=group),
        out_shape=(
            jax.ShapeDtypeStruct(held_shape, jnp.bfloat16),
            jax.ShapeDtypeStruct((span, kv_count * group * HEAD), jnp.bfloat16),
        ),
        in_specs=in_specs,
        out_specs=(anywhere, vmem),
        scratch_shapes=[
            pltpu.VMEM((2, rows, width), jnp.bfloat16),
            pltpu.VMEM((kv_count, 1, columns), jnp.float32),
            pltpu.VMEM((kv_count, 1, columns), jnp.float32),
            pltpu.VMEM((kv_count, HEAD, columns), jnp.float32),
            pltpu.SemaphoreType.DMA((blocks, 2)),
            pltpu.SemaphoreType.DMA((blocks, 2)),
        ],
        input_output_aliases={5: 0} if aliased else {},
        compiler_params=pltpu.CompilerParams(vmem_limit_bytes=40 * 1024 * 1024),
        cost_estimate=pl.CostEstimate(
            flops=4 * kv_count * columns * (rows + span) * HEAD,
            bytes_accessed=8 * rows * width,
            transcendentals=kv_count * columns * (rows + span),
        ),
    )(*operands)


def project_kernel(
    attended, weight, out, weight_blocks, outgoing, incoming, weight_sem, send_sem, recv_sem
):
    parts = weight_blocks.shape[0]
    own = lax.axis_index("tp")
    columns = out.shape[1]

    def load(step):
        part = lax.rem(own + step, parts)
        at = pl.ds(pl.multiple_of(part * columns, columns), columns)
        return pltpu.make_async_copy(
            weight.at[:, at], weight_blocks.at[step], weight_sem.at[step]
        )

    order = list(range(1, parts)) + [0]
    for step in order:
        load(step).start()
    barrier = pltpu.get_barrier_semaphore()
    for step in range(1, parts):
        pl.semaphore_signal(
            barrier,
            inc=1,
            device_id={"tp": lax.rem(own + step, parts)},
            device_id_type=pl.DeviceIdType.MESH,
        )

    def product(step):
        load(step).wait()
        return jnp.dot(
            attended[...], weight_blocks[step], preferred_element_type=jnp.float32
        )

    copies = []
    for step in range(1, parts):
        outgoing[step - 1] = product(step).astype(jnp.bfloat16)
        if step == 1:
            pl.semaphore_wait(barrier, parts - 1)
        copy = pltpu.make_async_remote_copy(
            src_ref=outgoing.at[step - 1],
            dst_ref=incoming.at[step - 1],
            send_sem=send_sem.at[step - 1],
            recv_sem=recv_sem.at[step - 1],
            device_id={"tp": lax.rem(own + step, parts)},
            device_id_type=pl.DeviceIdType.MESH,
        )
        copy.start()
        copies.append(copy)
    total = product(0)
    for step, copy in enumerate(copies):
        copy.wait_recv()
        total = total + incoming[step].astype(jnp.float32)
    out[...] = total.astype(jnp.bfloat16)
    for copy in copies:
        copy.wait_send()


def project(attended, out_weight, identity):
    parts = lax.axis_size("tp")
    rows, depth = attended.shape
    columns = out_weight.shape[1] // parts
    vmem = pl.BlockSpec(memory_space=pltpu.VMEM)
    return pl.pallas_call(
        project_kernel,
        out_shape=jax.ShapeDtypeStruct((rows, columns), jnp.bfloat16),
        in_specs=[vmem, pl.BlockSpec(memory_space=pl.ANY)],
        out_specs=vmem,
        scratch_shapes=[
            pltpu.VMEM((parts, depth, columns), jnp.bfloat16),
            pltpu.VMEM((parts - 1, rows, columns), jnp.bfloat16),
            pltpu.VMEM((parts - 1, rows, columns), jnp.bfloat16),
            pltpu.SemaphoreType.DMA((parts,)),
            pltpu.SemaphoreType.DMA((parts - 1,)),
            pltpu.SemaphoreType.DMA((parts - 1,)),
        ],
        compiler_params=pltpu.CompilerParams(
            collective_id=identity, has_side_effects=True, vmem_limit_bytes=40 * 1024 * 1024
        ),
        cost_estimate=pl.CostEstimate(
            flops=2 * rows * depth * columns * parts,
            bytes_accessed=2 * depth * columns * parts,
            transcendentals=0,
        ),
        name=f"project{identity}",
    )(attended, out_weight)


def on_device(queries, keys_new, values_new, caches, lengths, moving, destination, out_weight):
    replicas = lax.axis_size("rep")
    own_index = lax.axis_index("rep")
    slot_count, _, cache_rows, width = caches.shape
    span = queries.shape[0] // slot_count
    kv_count = width // HEAD
    group = queries.shape[1] // width
    leaving_slot = moving[own_index]
    staying_slot = 1 - leaving_slot
    leaving = lax.dynamic_index_in_dim(caches, leaving_slot, 0, keepdims=False)
    piece_rows = 2 * cache_rows // replicas
    pieces = leaving.reshape(replicas, piece_rows, width)
    spread = lax.all_to_all(pieces, "rep", split_axis=0, concat_axis=0, tiled=True)
    every = jnp.arange(replicas, dtype=jnp.int32)
    source_of = jnp.sum(
        jnp.where(destination[None, :] == every[:, None], every[None, :], 0), axis=1
    )
    ordered = jnp.take(spread, source_of, axis=0, mode="clip")
    arrived = lax.all_to_all(ordered, "rep", split_axis=0, concat_axis=0, tiled=True)
    arrived = arrived.reshape(1, 2, cache_rows, width)

    anchor = source_of[own_index]
    incoming_length = lengths[anchor, moving[anchor]]
    staying_length = lengths[own_index, staying_slot]
    query_t = (
        queries.reshape(slot_count, span, kv_count, group, HEAD)
        .transpose(0, 2, 4, 3, 1)
        .reshape(slot_count, kv_count, HEAD, group * span)
    )
    keys_by_slot = keys_new.reshape(slot_count, span, width)
    values_by_slot = values_new.reshape(slot_count, span, width)

    def pick(array, slot):
        return lax.dynamic_index_in_dim(array, slot, 0, keepdims=False)

    held, staying_attended = attend_slot(
        jnp.stack([staying_slot, staying_slot, staying_length]),
        caches,
        pick(query_t, staying_slot),
        pick(keys_by_slot, staying_slot),
        pick(values_by_slot, staying_slot),
        None,
        caches.shape,
    )
    staying_mixed = project(staying_attended, out_weight, 0)
    held, arrived_attended = attend_slot(
        jnp.stack([jnp.zeros_like(leaving_slot), leaving_slot, incoming_length]),
        arrived,
        pick(query_t, leaving_slot),
        pick(keys_by_slot, leaving_slot),
        pick(values_by_slot, leaving_slot),
        held,
        caches.shape,
    )
    arrived_mixed = project(arrived_attended, out_weight, 1)
    mixed = jnp.where(
        leaving_slot == 0,
        jnp.concatenate([arrived_mixed, staying_mixed], axis=0),
        jnp.concatenate([staying_mixed, arrived_mixed], axis=0),
    )
    return (mixed, held)


def solution(mesh):
    in_specs = (
        P("rep", "tp"),
        P("rep", "tp"),
        P("rep", "tp"),
        P("rep", None, None, "tp"),
        P(),
        P(),
        P(),
        P("tp", None),
    )
    out_specs = (P("rep", "tp"), P("rep", None, None, "tp"))
    return jax.shard_map(
        on_device, mesh=mesh, in_specs=in_specs, out_specs=out_specs, check_vma=False
    )
```

```python
import functools

import jax
import jax.numpy as jnp
from jax import lax
from jax.experimental import pallas as pl
from jax.experimental.pallas import tpu as pltpu
from jax.sharding import PartitionSpec as P

HEAD = 128
BLOCK = 512
LOG2E = 1.4426950408889634
masked_score = -1e30


def slot_kernel(
    scalars, source, query_t, keys_fresh, values_fresh, *rest, aliased, kv_count, group
):
    if aliased:
        rest = rest[1:]
    held, attended, cache, row_max, row_total, weighted, in_sem, out_sem = rest
    taken, target, length = scalars[0], scalars[1], scalars[2]
    rows = cache.shape[1]
    blocks = rows // BLOCK
    span = keys_fresh.shape[0]
    factor = HEAD ** (-0.5) * LOG2E

    def fetch(block, part):
        at = pl.ds(pl.multiple_of(block * BLOCK, BLOCK), BLOCK)
        return pltpu.make_async_copy(
            source.at[taken, part, at], cache.at[part, at], in_sem.at[block, part]
        )

    def put(block, part):
        at = pl.ds(pl.multiple_of(block * BLOCK, BLOCK), BLOCK)
        return pltpu.make_async_copy(
            cache.at[part, at], held.at[target, part, at], out_sem.at[block, part]
        )

    for block in range(blocks):
        for part in range(2):
            fetch(block, part).start()

    def scores_of(head, keys):
        return lax.dot_general(
            keys,
            query_t[head],
            (((1,), (0,)), ((), ())),
            preferred_element_type=jnp.float32,
        )

    def mix(values, weights):
        return lax.dot_general(
            values,
            weights.astype(jnp.bfloat16),
            (((0,), (0,)), ((), ())),
            preferred_element_type=jnp.float32,
        )

    key_at = lax.broadcasted_iota(jnp.int32, (span, group * span), 0)
    token_at = lax.broadcasted_iota(jnp.int32, (span, group * span), 1) % span
    for head in range(kv_count):
        lanes = slice(head * HEAD, (head + 1) * HEAD)
        scores = jnp.where(
            key_at <= token_at, scores_of(head, keys_fresh[:, lanes]), masked_score
        )
        new_max = jnp.max(scores, axis=0, keepdims=True)
        weights = jnp.exp2((scores - new_max) * factor)
        row_max[head] = new_max
        row_total[head] = jnp.sum(weights, axis=0, keepdims=True)
        weighted[head] = mix(values_fresh[:, lanes], weights)

    def absorb(block, masked):
        start = pl.multiple_of(block * BLOCK, BLOCK)
        at = pl.ds(start, BLOCK)
        for head in range(kv_count):
            lanes = slice(head * HEAD, (head + 1) * HEAD)
            scores = scores_of(head, cache[0, at, lanes])
            if masked:
                position = start + lax.broadcasted_iota(jnp.int32, scores.shape, 0)
                scores = jnp.where(position < length, scores, masked_score)
            old_max = row_max[head]
            new_max = jnp.maximum(old_max, jnp.max(scores, axis=0, keepdims=True))
            rescale = jnp.exp2((old_max - new_max) * factor)
            weights = jnp.exp2((scores - new_max) * factor)
            row_max[head] = new_max
            row_total[head] = row_total[head] * rescale + jnp.sum(
                weights, axis=0, keepdims=True
            )
            weighted[head] = weighted[head] * rescale + mix(cache[1, at, lanes], weights)

    def step(block, carry):
        for part in range(2):
            fetch(block, part).wait()
            put(block, part).start()
        start = block * BLOCK

        @pl.when(start + BLOCK <= length)
        def _():
            absorb(block, False)

        @pl.when((start < length) & (length < start + BLOCK))
        def _():
            absorb(block, True)

        return carry

    lax.fori_loop(0, blocks, step, 0)
    for head in range(kv_count):
        result = (weighted[head] / row_total[head]).T
        for member in range(group):
            lanes = slice((head * group + member) * HEAD, (head * group + member + 1) * HEAD)
            attended[:, lanes] = result[member * span : (member + 1) * span].astype(
                jnp.bfloat16
            )
    for block in range(blocks):
        for part in range(2):
            put(block, part).wait()


def attend_slot(scalars, source, query_t, keys_fresh, values_fresh, held, held_shape):
    kv_count, _, columns = query_t.shape
    span = keys_fresh.shape[0]
    group = columns // span
    rows, width = source.shape[2:]
    aliased = held is not None
    anywhere = pl.BlockSpec(memory_space=pl.ANY)
    vmem = pl.BlockSpec(memory_space=pltpu.VMEM)
    operands = [scalars, source, query_t, keys_fresh, values_fresh]
    in_specs = [pl.BlockSpec(memory_space=pltpu.SMEM), anywhere, vmem, vmem, vmem]
    if aliased:
        operands.append(held)
        in_specs.append(anywhere)
    blocks = rows // BLOCK
    return pl.pallas_call(
        functools.partial(slot_kernel, aliased=aliased, kv_count=kv_count, group=group),
        out_shape=(
            jax.ShapeDtypeStruct(held_shape, jnp.bfloat16),
            jax.ShapeDtypeStruct((span, kv_count * group * HEAD), jnp.bfloat16),
        ),
        in_specs=in_specs,
        out_specs=(anywhere, vmem),
        scratch_shapes=[
            pltpu.VMEM((2, rows, width), jnp.bfloat16),
            pltpu.VMEM((kv_count, 1, columns), jnp.float32),
            pltpu.VMEM((kv_count, 1, columns), jnp.float32),
            pltpu.VMEM((kv_count, HEAD, columns), jnp.float32),
            pltpu.SemaphoreType.DMA((blocks, 2)),
            pltpu.SemaphoreType.DMA((blocks, 2)),
        ],
        input_output_aliases={5: 0} if aliased else {},
        compiler_params=pltpu.CompilerParams(vmem_limit_bytes=60 * 1024 * 1024),
        cost_estimate=pl.CostEstimate(
            flops=4 * kv_count * columns * (rows + span) * HEAD,
            bytes_accessed=8 * rows * width,
            transcendentals=kv_count * columns * (rows + span),
        ),
    )(*operands)


def project_kernel(
    attended, weight, out, weight_blocks, outgoing, incoming, weight_sem, send_sem, recv_sem
):
    parts = weight_blocks.shape[0]
    own = lax.axis_index("tp")
    columns = out.shape[1]

    def load(step):
        part = lax.rem(own + step, parts)
        at = pl.ds(pl.multiple_of(part * columns, columns), columns)
        return pltpu.make_async_copy(
            weight.at[:, at], weight_blocks.at[step], weight_sem.at[step]
        )

    order = list(range(1, parts)) + [0]
    for step in order:
        load(step).start()
    barrier = pltpu.get_barrier_semaphore()
    for step in range(1, parts):
        pl.semaphore_signal(
            barrier,
            inc=1,
            device_id={"tp": lax.rem(own + step, parts)},
            device_id_type=pl.DeviceIdType.MESH,
        )

    def product(step):
        load(step).wait()
        return jnp.dot(
            attended[...], weight_blocks[step], preferred_element_type=jnp.float32
        )

    copies = []
    for step in range(1, parts):
        outgoing[step - 1] = product(step).astype(jnp.bfloat16)
        if step == 1:
            pl.semaphore_wait(barrier, parts - 1)
        copy = pltpu.make_async_remote_copy(
            src_ref=outgoing.at[step - 1],
            dst_ref=incoming.at[step - 1],
            send_sem=send_sem.at[step - 1],
            recv_sem=recv_sem.at[step - 1],
            device_id={"tp": lax.rem(own + step, parts)},
            device_id_type=pl.DeviceIdType.MESH,
        )
        copy.start()
        copies.append(copy)
    total = product(0)
    for step, copy in enumerate(copies):
        copy.wait_recv()
        total = total + incoming[step].astype(jnp.float32)
    out[...] = total.astype(jnp.bfloat16)
    for copy in copies:
        copy.wait_send()


def project(attended, out_weight, identity):
    parts = lax.axis_size("tp")
    rows, depth = attended.shape
    columns = out_weight.shape[1] // parts
    vmem = pl.BlockSpec(memory_space=pltpu.VMEM)
    return pl.pallas_call(
        project_kernel,
        out_shape=jax.ShapeDtypeStruct((rows, columns), jnp.bfloat16),
        in_specs=[vmem, pl.BlockSpec(memory_space=pl.ANY)],
        out_specs=vmem,
        scratch_shapes=[
            pltpu.VMEM((parts, depth, columns), jnp.bfloat16),
            pltpu.VMEM((parts - 1, rows, columns), jnp.bfloat16),
            pltpu.VMEM((parts - 1, rows, columns), jnp.bfloat16),
            pltpu.SemaphoreType.DMA((parts,)),
            pltpu.SemaphoreType.DMA((parts - 1,)),
            pltpu.SemaphoreType.DMA((parts - 1,)),
        ],
        compiler_params=pltpu.CompilerParams(
            collective_id=identity, has_side_effects=True, vmem_limit_bytes=60 * 1024 * 1024
        ),
        cost_estimate=pl.CostEstimate(
            flops=2 * rows * depth * columns * parts,
            bytes_accessed=2 * depth * columns * parts,
            transcendentals=0,
        ),
        name=f"project{identity}",
    )(attended, out_weight)


def on_device(queries, keys_new, values_new, caches, lengths, moving, destination, out_weight):
    replicas = lax.axis_size("rep")
    own_index = lax.axis_index("rep")
    slot_count, _, cache_rows, width = caches.shape
    span = queries.shape[0] // slot_count
    kv_count = width // HEAD
    group = queries.shape[1] // width
    leaving_slot = moving[own_index]
    staying_slot = 1 - leaving_slot
    leaving = lax.dynamic_index_in_dim(caches, leaving_slot, 0, keepdims=False)
    piece_rows = 2 * cache_rows // replicas
    pieces = leaving.reshape(replicas, piece_rows, width)
    destination, pieces = lax.optimization_barrier((destination, pieces))
    spread = lax.all_to_all(pieces, "rep", split_axis=0, concat_axis=0, tiled=True)
    every = jnp.arange(replicas, dtype=jnp.int32)
    source_of = jnp.sum(
        jnp.where(destination[None, :] == every[:, None], every[None, :], 0), axis=1
    )
    anchor = source_of[own_index]
    incoming_length = lengths[anchor, moving[anchor]]
    staying_length = lengths[own_index, staying_slot]
    query_t = (
        queries.reshape(slot_count, span, kv_count, group, HEAD)
        .transpose(0, 2, 4, 3, 1)
        .reshape(slot_count, kv_count, HEAD, group * span)
    )
    keys_by_slot = keys_new.reshape(slot_count, span, width)
    values_by_slot = values_new.reshape(slot_count, span, width)

    def pick(array, slot):
        return lax.dynamic_index_in_dim(array, slot, 0, keepdims=False)

    held, staying_attended = attend_slot(
        jnp.stack([staying_slot, staying_slot, staying_length]),
        caches,
        pick(query_t, staying_slot),
        pick(keys_by_slot, staying_slot),
        pick(values_by_slot, staying_slot),
        None,
        caches.shape,
    )
    spread, staying_attended = lax.optimization_barrier((spread, staying_attended))
    ordered = jnp.take(spread, source_of, axis=0, mode="clip")
    arrived = lax.all_to_all(ordered, "rep", split_axis=0, concat_axis=0, tiled=True)
    arrived = arrived.reshape(1, 2, cache_rows, width)
    staying_mixed = project(staying_attended, out_weight, 0)
    held, arrived_attended = attend_slot(
        jnp.stack([jnp.zeros_like(leaving_slot), leaving_slot, incoming_length]),
        arrived,
        pick(query_t, leaving_slot),
        pick(keys_by_slot, leaving_slot),
        pick(values_by_slot, leaving_slot),
        held,
        caches.shape,
    )
    arrived_mixed = project(arrived_attended, out_weight, 1)
    mixed = jnp.where(
        leaving_slot == 0,
        jnp.concatenate([arrived_mixed, staying_mixed], axis=0),
        jnp.concatenate([staying_mixed, arrived_mixed], axis=0),
    )
    return (mixed, held)


def solution(mesh):
    in_specs = (
        P("rep", "tp"),
        P("rep", "tp"),
        P("rep", "tp"),
        P("rep", None, None, "tp"),
        P(),
        P(),
        P(),
        P("tp", None),
    )
    out_specs = (P("rep", "tp"), P("rep", None, None, "tp"))
    return jax.shard_map(
        on_device, mesh=mesh, in_specs=in_specs, out_specs=out_specs, check_vma=False
    )
```
